32 devices in a mesh: samp: 16 (over z, y, core), feat: 2 (over x).
Axes of the slice: x: 2, y: 2, z: 4, core: 2. Of those that a mesh axis runs over, the one named last changes fastest.
Arguments:
- grads: bfloat16 [8192, 4096], P('samp', 'feat'), may hold values from -60 to 60
- weights: float32 [8192], P('samp'), may hold values from 0.05 to 6
- targets: float32 [4096, 64], P('feat'), may hold values from -6 to 6
Outputs:
- scores: float32 [8192, 64], P(('samp', 'feat'))
- solution: float32 [4096, 64], P('feat')
- residual: float32 [4096, 64], P('feat')
The draws below stay inside these ranges and needn't reach their ends.
All inputs are finite; a program needn't handle non-finite values.
Results may differ from the reference program's by a relative error of at most 0.014.
Values may be sent and summed in bfloat16 or wider, within the bound.
A program may use at most 64 MiB of HBM per device.

```python
import math
import jax
import jax.numpy as jnp
from jax import lax

FEATURES = 4096
DIRS = 64
ITERS = 2
SAMPLES = 8192


def draw_grads(key, part):
    first = jax.random.fold_in(key, 11)
    second = jax.random.fold_in(key, 12)
    ramp = 1.0 + 2.0 * jnp.arange(FEATURES, dtype=jnp.float32) / FEATURES
    column_scale = jnp.exp(jax.random.uniform(second, (FEATURES,), jnp.float32, math.log(0.1), math.log(3.0))) * ramp
    base = jax.random.normal(first, (SAMPLES, FEATURES), jnp.float32)
    return (base * column_scale[None, :]).astype(jnp.bfloat16)


def draw_weights(key, part):
    first = jax.random.fold_in(key, 21)
    ramp = 1.0 + 2.0 * jnp.arange(SAMPLES, dtype=jnp.float32) / SAMPLES
    base = jnp.exp(jax.random.uniform(first, (SAMPLES,), jnp.float32, math.log(0.05), math.log(2.0)))
    return base * ramp


def block_scale(own_key, dims, shards, low, high):
    def one(position, parts):
        heights = jax.random.uniform(jax.random.fold_in(jax.random.fold_in(own_key, 6), position), (parts,), jnp.float32, low / len(shards), high / len(shards))
        return jnp.repeat(jnp.exp(heights), dims[position] // parts).reshape((-1,) + (1,) * (len(dims) - position - 1))

    factor_of = one(*shards[0])
    for cut in shards[1:]:
        factor_of = factor_of * one(*cut)
    return factor_of


def normal_values(stream_key, dims, deviation, limit, cuts=(), kind=jnp.bfloat16):
    loudness = block_scale(stream_key, dims, cuts, -0.22, 0.18) if cuts else 1.0
    entries = jax.random.normal(stream_key, dims, jnp.float32) * deviation * loudness
    return jnp.minimum(jnp.maximum(entries, -limit), limit).astype(kind)


def setup_inputs(seed: int = 0) -> dict:
    keys = jax.random.split(jax.random.key(seed), 4)
    return {
        "grads": draw_grads(jax.random.fold_in(keys[3], 71), 0),
        "weights": draw_weights(jax.random.fold_in(keys[3], 71), 0),
        "targets": normal_values(keys[2], (FEATURES, DIRS), 1.0, 6.0, ((0, 2),), jnp.float32),
    }


damping_term = 0.1

def apply_operator(grads, weights, vector):
    packed = vector.astype(jnp.bfloat16)
    sample_rows = jnp.dot(grads, packed, preferred_element_type=jnp.float32)
    weighted = (sample_rows * (weights / SAMPLES)[:, None]).astype(jnp.bfloat16)
    image = lax.dot_general(grads, weighted, (((0,), (0,)), ((), ())), preferred_element_type=jnp.float32)
    return (sample_rows, image + damping_term * vector)

def reference(grads, weights, targets):
    solution = jnp.zeros_like(targets)
    resid = targets
    direction = targets
    accum = jnp.zeros((grads.shape[0], targets.shape[1]), jnp.float32)
    norm_now = lax.optimization_barrier(jnp.sum(resid * resid, axis=0))
    for step in range(ITERS):
        sample_rows, image = apply_operator(grads, weights, direction)
        alpha = norm_now / lax.optimization_barrier(jnp.sum(direction * image, axis=0))
        solution = solution + alpha * direction
        resid = resid - alpha * image
        accum = accum + alpha * sample_rows
        if step + 1 < ITERS:
            norm_next = lax.optimization_barrier(jnp.sum(resid * resid, axis=0))
            direction = resid + norm_next / norm_now * direction
            norm_now = norm_next
    scores = accum / math.sqrt(FEATURES)
    return (scores, solution, resid)
```

```python
import functools
import math

import jax
import jax.numpy as jnp
from jax import lax
from jax.experimental import pallas as pl
from jax.experimental.pallas import tpu as pltpu
from jax.sharding import PartitionSpec as P

ITERS = 2
LANES = 128
MESH = pl.DeviceIdType.MESH

damping_term = 0.1


def pack_columns(columns):
    dirs = columns[0].shape[0]
    lane = lax.broadcasted_iota(jnp.int32, (dirs, LANES), 1)
    tile = jnp.zeros((dirs, LANES), jnp.float32)
    for position, column in enumerate(columns):
        tile = jnp.where(lane == position, column, tile)
    if dirs < LANES:
        tile = jnp.concatenate([tile, jnp.zeros((LANES - dirs, LANES), jnp.float32)], axis=0)
    return tile.T[:8]


def unpack_columns(tile, count, dirs):
    padded = jnp.concatenate([tile, jnp.zeros((LANES - 8, LANES), jnp.float32)], axis=0).T
    return [padded[:dirs, i : i + 1] for i in range(count)]


def kernel(
    chips, total, full_width,
    grads_ref, weights_ref, targets_ref,
    scores_ref, solution_ref, resid_ref,
    rows_out, rows_in, tile_out, tile_in,
    image_f32, image_b16, pair_in, pair_tile_out, pair_tile_in,
    chip_out, chip_in, chip_tiles, gathered,
    feat_send, feat_recv, pair_send, pair_recv, chip_send, chip_recv,
):
    samp, feat = lax.axis_index("samp"), lax.axis_index("feat")
    core = lax.rem(samp, 2)
    chip = lax.div(samp, 2)
    dirs, width = targets_ref.shape
    rows_dev = grads_ref.shape[0]
    partner = (samp + 1 - 2 * core, feat)
    mirror = (samp, 1 - feat)

    def peer(offset):
        other = lax.rem(chip + offset, chips)
        return other, (other * 2 + core, feat)

    barrier = pltpu.get_barrier_semaphore()
    for device in [partner, mirror] + [peer(d)[1] for d in range(1, chips)]:
        pl.semaphore_signal(barrier, inc=1, device_id=device, device_id_type=MESH)

    def remote(src, dst, send, recv, device):
        return pltpu.make_async_remote_copy(
            src_ref=src, dst_ref=dst, send_sem=send, recv_sem=recv, device_id=device, device_id_type=MESH
        )

    scaled = weights_ref[...] / total
    own_lanes = pl.ds(pl.multiple_of((core * chips + chip) * LANES, LANES), LANES)
    target_slice = targets_ref[:, own_lanes]

    for step in range(ITERS):
        targets = targets_ref[...]
        if step == 0:
            packed = targets.astype(jnp.bfloat16)
            sums = [jnp.sum(targets * targets, axis=1, keepdims=True)]
        else:
            packed = jnp.concatenate(
                [gathered[step - 1, c, i] for c in range(2) for i in range(chips)], axis=1
            )
            wide = packed.astype(jnp.float32)
            sums = [
                jnp.sum(wide * wide, axis=1, keepdims=True),
                jnp.sum(wide * targets, axis=1, keepdims=True),
            ]
        own = lax.dot_general(
            packed, grads_ref[...], (((1,), (1,)), ((), ())), preferred_element_type=jnp.float32
        )
        rows_out[step] = own.astype(jnp.bfloat16)
        tile_out[step] = pack_columns(sums)
        if step == 0:
            pl.semaphore_wait(barrier, chips + 1)
        copies = [
            remote(rows_out.at[step], rows_in.at[step], feat_send.at[step, 0], feat_recv.at[step, 0], mirror),
            remote(tile_out.at[step], tile_in.at[step], feat_send.at[step, 1], feat_recv.at[step, 1], mirror),
        ]
        for copy in copies:
            copy.start()
        for copy in copies:
            copy.wait()
        rows = own + rows_in[step].astype(jnp.float32)
        sums = unpack_columns(tile_out[step] + tile_in[step], len(sums), dirs)
        if step == 0:
            norm = square = sums[0]
            resid_slice = target_slice
            direction_slice = target_slice
            first_rows = rows
            first_norm = norm
        else:
            norm = sums[0]
            ratio = norm / first_norm
            square = norm + 2.0 * ratio * sums[1] + ratio * ratio * first_norm
            rows = rows + ratio * first_rows
            direction_slice = resid_slice + ratio * target_slice
        weighted = (rows * scaled).astype(jnp.bfloat16)
        curve = jnp.sum(weighted.astype(jnp.float32) * rows, axis=1, keepdims=True)
        image = jnp.dot(weighted, grads_ref[...], preferred_element_type=jnp.float32)
        for c in range(2):
            for i in range(chips):
                at = (c * chips + i) * LANES
                block = image[:, at : at + LANES]
                image_f32[c, i] = block
                image_b16[step, c, i] = block.astype(jnp.bfloat16)
        pair_tile_out[step] = pack_columns([curve])
        copies = [
            remote(image_b16.at[step, 1 - core], pair_in.at[step], pair_send.at[step, 0], pair_recv.at[step, 0], partner),
            remote(pair_tile_out.at[step], pair_tile_in.at[step], pair_send.at[step, 1], pair_recv.at[step, 1], partner),
        ]
        for copy in copies:
            copy.start()
        for copy in copies:
            copy.wait()
        image_f32[core] = image_f32[core] + pair_in[step].astype(jnp.float32)
        chip_out[step] = image_f32[core].astype(jnp.bfloat16)
        chip_tiles[step, chip] = pair_tile_out[step] + pair_tile_in[step]
        sends = []
        for d in range(1, chips):
            other, device = peer(d)
            sends.append(remote(
                chip_out.at[step, other], chip_in.at[step, chip],
                chip_send.at[step, 0, d], chip_recv.at[step, 0, chip], device))
            sends.append(remote(
                chip_tiles.at[step, chip], chip_tiles.at[step, chip],
                chip_send.at[step, 1, d], chip_recv.at[step, 1, chip], device))
        for copy in sends:
            copy.start()
        reduced = image_f32[core, chip]
        for d in range(1, chips):
            other, device = peer(d)
            remote(
                chip_out.at[step, other], chip_in.at[step, other],
                chip_send.at[step, 0, d], chip_recv.at[step, 0, other], device).wait_recv()
            reduced = reduced + chip_in[step, other].astype(jnp.float32)
            remote(
                chip_tiles.at[step, other], chip_tiles.at[step, other],
                chip_send.at[step, 1, d], chip_recv.at[step, 1, other], device).wait_recv()
        curve_tile = chip_tiles[step, 0]
        for i in range(1, chips):
            curve_tile = curve_tile + chip_tiles[step, i]
        curvature = unpack_columns(curve_tile, 1, dirs)[0] + damping_term * square
        alpha = norm / curvature
        resid_slice = resid_slice - alpha * (reduced + damping_term * direction_slice)
        gathered[step, core, chip] = resid_slice.astype(jnp.bfloat16)
        spread = []
        for d in range(1, chips):
            other, device = peer(d)
            spread.append(remote(
                gathered.at[step, core, chip], gathered.at[step, core, chip],
                chip_send.at[step, 2, d], chip_recv.at[step, 2, chip], device))
        for copy in spread:
            copy.start()
        if step == 0:
            first_alpha = alpha
        else:
            scores = (first_alpha * first_rows + alpha * rows) / math.sqrt(full_width)
            share = rows_dev // 2
            scores_ref[...] = jnp.where(feat == 0, scores[:, :share], scores[:, share:])
            solution_ref[...] = first_alpha * targets + alpha * (wide + ratio * targets)
        for copy in sends:
            copy.wait_send()
        for d in range(1, chips):
            other, device = peer(d)
            remote(
                gathered.at[step, core, other], gathered.at[step, core, other],
                chip_send.at[step, 2, d], chip_recv.at[step, 2, other], device).wait_recv()
        swap = remote(
            gathered.at[step, core], gathered.at[step, core],
            pair_send.at[step, 2], pair_recv.at[step, 2], partner)
        swap.start()
        for copy in spread:
            copy.wait_send()
        swap.wait_send()
        remote(
            gathered.at[step, 1 - core], gathered.at[step, 1 - core],
            pair_send.at[step, 2], pair_recv.at[step, 2], partner).wait_recv()
    for c in range(2):
        for i in range(chips):
            at = (c * chips + i) * LANES
            resid_ref[:, at : at + LANES] = gathered[ITERS - 1, c, i].astype(jnp.float32)


def fused(grads, weights, targets):
    rows_dev, feat_cols = grads.shape
    n_samp = lax.axis_size("samp")
    n_feat = lax.axis_size("feat")
    dirs = targets.shape[1]
    chips = n_samp // 2
    f32, b16 = jnp.float32, jnp.bfloat16
    vmem = pl.BlockSpec(memory_space=pltpu.VMEM)
    dma = pltpu.SemaphoreType.DMA
    scores, solved, resid = pl.pallas_call(
        functools.partial(kernel, chips, rows_dev * n_samp, feat_cols * n_feat),
        out_shape=(
            jax.ShapeDtypeStruct((dirs, rows_dev // n_feat), f32),
            jax.ShapeDtypeStruct((dirs, feat_cols), f32),
            jax.ShapeDtypeStruct((dirs, feat_cols), f32),
        ),
        in_specs=[vmem] * 3,
        out_specs=[vmem] * 3,
        scratch_shapes=[
            pltpu.VMEM((ITERS, dirs, rows_dev), b16),
            pltpu.VMEM((ITERS, dirs, rows_dev), b16),
            pltpu.VMEM((ITERS, 8, LANES), f32),
            pltpu.VMEM((ITERS, 8, LANES), f32),
            pltpu.VMEM((2, chips, dirs, LANES), f32),
            pltpu.VMEM((ITERS, 2, chips, dirs, LANES), b16),
            pltpu.VMEM((ITERS, chips, dirs, LANES), b16),
            pltpu.VMEM((ITERS, 8, LANES), f32),
            pltpu.VMEM((ITERS, 8, LANES), f32),
            pltpu.VMEM((ITERS, chips, dirs, LANES), b16),
            pltpu.VMEM((ITERS, chips, dirs, LANES), b16),
            pltpu.VMEM((ITERS, chips, 8, LANES), f32),
            pltpu.VMEM((ITERS, 2, chips, dirs, LANES), b16),
            dma((ITERS, 2)), dma((ITERS, 2)),
            dma((ITERS, 3)), dma((ITERS, 3)),
            dma((ITERS, 3, chips)), dma((ITERS, 3, chips)),
        ],
        compiler_params=pltpu.CompilerParams(collective_id=0, has_side_effects=True),
        name="cg",
    )(grads, weights[None, :], targets.T)
    return scores.T, solved.T, resid.T


def per_device(grads, weights, targets):
    rows_dev, feat_cols = grads.shape
    n_samp = lax.axis_size("samp")
    n_feat = lax.axis_size("feat")
    total = rows_dev * n_samp
    full_width = feat_cols * n_feat
    share = rows_dev // n_feat
    offset = lax.axis_index("feat") * share
    scaled = weights / total
    regrouped = lax.all_to_all(grads, "feat", split_axis=0, concat_axis=1, tiled=True)
    own_weights = lax.dynamic_slice_in_dim(scaled, offset, share, 0)

    def column_norms(resid):
        squares = jnp.sum(resid * resid, axis=0)
        parts = (squares,)
        return lax.psum((parts[0],), "feat")

    solution = jnp.zeros_like(targets)
    resid = targets
    direction = targets
    accum = jnp.zeros((share, targets.shape[1]), jnp.float32)
    norm_now = column_norms(resid)[0]
    for step in range(ITERS):
        packed = direction.astype(jnp.bfloat16)
        sample_rows = jnp.dot(
            regrouped,
            lax.all_gather(packed, "feat", axis=0, tiled=True),
            preferred_element_type=jnp.float32,
        )
        weighted = (sample_rows * own_weights[:, None]).astype(jnp.bfloat16)
        partial_image = lax.psum_scatter(
            lax.dot_general(
                regrouped, weighted, (((0,), (0,)), ((), ())), preferred_element_type=jnp.float32
            ).astype(jnp.bfloat16),
            "feat",
            scatter_dimension=0,
            tiled=True,
        ).astype(jnp.float32)
        own_rows = sample_rows
        apply_own_weights = own_weights
        image = lax.psum(partial_image, "samp") + damping_term * direction
        own_rows, own_weights, image = (own_rows, apply_own_weights, image)
        curvature = lax.psum(jnp.sum(direction * image, axis=0), "feat")
        alpha = norm_now / curvature
        solution = solution + alpha * direction
        resid = resid - alpha * image
        accum = accum + alpha * own_rows
        if step + 1 < ITERS:
            sums = column_norms(resid)
            norm_next = sums[0]
            ratio = norm_next / norm_now
            direction = resid + ratio * direction
            norm_now = norm_next
    scores = accum / math.sqrt(full_width)
    return (scores, solution, resid)


def dispatch(grads, weights, targets):
    rows_dev, feat_cols = grads.shape
    n_samp, n_feat = lax.axis_size("samp"), lax.axis_size("feat")
    fits = (
        n_feat == 2
        and n_samp % 2 == 0
        and n_samp >= 4
        and feat_cols == n_samp * LANES
        and rows_dev % (2 * LANES) == 0
        and targets.shape[1] % 16 == 0
        and targets.shape[1] <= LANES
    )
    return (fused if fits else per_device)(grads, weights, targets)


def solution(mesh):
    return jax.shard_map(
        dispatch,
        mesh=mesh,
        in_specs=(P("samp", "feat"), P("samp"), P("feat", None)),
        out_specs=(P(("samp", "feat"), None), P("feat", None), P("feat", None)),
        check_vma=False,
    )
```

```python
import functools
import math

import jax
import jax.numpy as jnp
from jax import lax
from jax.experimental import pallas as pl
from jax.experimental.pallas import tpu as pltpu
from jax.sharding import PartitionSpec as P

ITERS = 2
LANES = 128
VMEM_BYTES = 16 * 2**20
MESH = pl.DeviceIdType.MESH

damping_term = 0.1


def pack_columns(columns):
    dirs = columns[0].shape[0]
    lane = lax.broadcasted_iota(jnp.int32, (dirs, LANES), 1)
    tile = jnp.zeros((dirs, LANES), jnp.float32)
    for position, column in enumerate(columns):
        tile = jnp.where(lane == position, column, tile)
    if dirs < LANES:
        tile = jnp.concatenate([tile, jnp.zeros((LANES - dirs, LANES), jnp.float32)], axis=0)
    return tile.T[:8]


def unpack_columns(tile, count, dirs):
    padded = jnp.concatenate([tile, jnp.zeros((LANES - 8, LANES), jnp.float32)], axis=0).T
    return [padded[:dirs, i : i + 1] for i in range(count)]


def kernel(
    chips, total, full_width,
    grads_ref, weights_ref, targets_ref,
    scores_ref, solution_ref, resid_ref,
    rows_out, rows_in, tile_out, tile_in,
    image_f32, image_b16, pair_in, pair_tile_out, pair_tile_in,
    chip_out, chip_in, chip_tiles, gathered,
    feat_send, feat_recv, pair_send, pair_recv, chip_send, chip_recv,
):
    samp, feat = lax.axis_index("samp"), lax.axis_index("feat")
    core = lax.rem(samp, 2)
    chip = lax.div(samp, 2)
    dirs, width = targets_ref.shape
    rows_dev = grads_ref.shape[0]
    half = rows_dev // 2
    partner = (samp + 1 - 2 * core, feat)
    mirror = (samp, 1 - feat)
    wide_half = chips * LANES

    def peer(offset):
        other = lax.rem(chip + offset, chips)
        return other, (other * 2 + core, feat)

    barrier = pltpu.get_barrier_semaphore()
    for device in [partner, mirror] + [peer(d)[1] for d in range(1, chips)]:
        pl.semaphore_signal(barrier, inc=1, device_id=device, device_id_type=MESH)

    def remote(src, dst, send, recv, device):
        return pltpu.make_async_remote_copy(
            src_ref=src, dst_ref=dst, send_sem=send, recv_sem=recv, device_id=device, device_id_type=MESH
        )

    def lanes_of(which):
        return pl.ds(pl.multiple_of(which * wide_half, wide_half), wide_half)

    own_half, other_half = lanes_of(core), lanes_of(1 - core)
    own_lanes = pl.ds(pl.multiple_of((core * chips + chip) * LANES, LANES), LANES)
    nt = (((1,), (1,)), ((), ()))

    def joined(step, which):
        return jnp.concatenate([gathered[step, which, i] for i in range(chips)], axis=1)

    for step in range(ITERS):
        mine = []
        copies = []
        if step == 0:
            targets = targets_ref[...]
            packed = targets.astype(jnp.bfloat16)
        else:
            near = joined(step - 1, core)
            started = [
                lax.dot_general(
                    near, grads_ref[h * half : (h + 1) * half, own_half], nt,
                    preferred_element_type=jnp.float32)
                for h in range(2)
            ]
            for i in range(chips):
                remote(
                    gathered.at[step - 1, 1 - core, i], gathered.at[step - 1, 1 - core, i],
                    pair_send.at[step - 1, 2 + i], pair_recv.at[step - 1, 2 + i], partner).wait_recv()
            far = joined(step - 1, 1 - core)
        for h in range(2):
            rows_h = slice(h * half, (h + 1) * half)
            if step == 0:
                part = lax.dot_general(
                    packed, grads_ref[rows_h, :], nt, preferred_element_type=jnp.float32)
            else:
                part = started[h] + lax.dot_general(
                    far, grads_ref[rows_h, other_half], nt, preferred_element_type=jnp.float32)
            rows_out[step, h] = part.astype(jnp.bfloat16)
            if step == 0 and h == 0:
                pl.semaphore_wait(barrier, chips + 1)
            copies.append(remote(
                rows_out.at[step, h], rows_in.at[step, h],
                feat_send.at[step, h], feat_recv.at[step, h], mirror))
            copies[-1].start()
            mine.append(part)
        if step == 0:
            sums = [jnp.sum(targets * targets, axis=1, keepdims=True)]
        else:
            pieces = [(near, own_half), (far, other_half)]
            sums = [0.0, 0.0]
            for block, lanes in pieces:
                block = block.astype(jnp.float32)
                sums[0] = sums[0] + jnp.sum(block * block, axis=1, keepdims=True)
                sums[1] = sums[1] + jnp.sum(block * targets_ref[:, lanes], axis=1, keepdims=True)
        tile_out[step] = pack_columns(sums)
        copies.append(remote(tile_out.at[step], tile_in.at[step], feat_send.at[step, 2], feat_recv.at[step, 2], mirror))
        copies[-1].start()
        if step == 0:
            scaled = weights_ref[...] / total
            target_slice = targets_ref[:, own_lanes]

        def finish_sums():
            copies[2].wait()
            return unpack_columns(tile_out[step] + tile_in[step], len(sums), dirs)

        if step == 1:
            sums = finish_sums()
            norm = sums[0]
            ratio = norm / first_norm
            square = norm + 2.0 * ratio * sums[1] + ratio * ratio * first_norm
            direction_slice = resid_slice + ratio * target_slice
        rows, curve = [], 0.0
        toward = mine_image = None
        for h in range(2):
            rows_h = slice(h * half, (h + 1) * half)
            copies[h].wait()
            whole = mine[h] + rows_in[step, h].astype(jnp.float32)
            if step == 1:
                whole = whole + ratio * first_rows[h]
            rows.append(whole)
            weighted = (whole * scaled[:, rows_h]).astype(jnp.bfloat16)
            there = jnp.dot(weighted, grads_ref[rows_h, other_half], preferred_element_type=jnp.float32)
            toward = there if h == 0 else toward + there
            if h == 1:
                for i in range(chips):
                    image_b16[step, i] = toward[:, i * LANES : (i + 1) * LANES].astype(jnp.bfloat16)
                swap = remote(image_b16.at[step], pair_in.at[step], pair_send.at[step, 0], pair_recv.at[step, 0], partner)
                swap.start()
            curve = curve + jnp.sum(weighted.astype(jnp.float32) * whole, axis=1, keepdims=True)
            if h == 1:
                pair_tile_out[step] = pack_columns([curve])
                swap_tile = remote(
                    pair_tile_out.at[step], pair_tile_in.at[step], pair_send.at[step, 1], pair_recv.at[step, 1], partner)
                swap_tile.start()
            here = jnp.dot(weighted, grads_ref[rows_h, own_half], preferred_element_type=jnp.float32)
            mine_image = here if h == 0 else mine_image + here
        if step == 0:
            first_rows = rows
            sums = finish_sums()
            first_norm = norm = square = sums[0]
            resid_slice = direction_slice = target_slice
        swap_tile.wait()
        chip_tiles[step, chip] = pair_tile_out[step] + pair_tile_in[step]
        sends = []
        for d in range(1, chips):
            other, device = peer(d)
            sends.append(remote(
                chip_tiles.at[step, chip], chip_tiles.at[step, chip],
                chip_send.at[step, 1, d], chip_recv.at[step, 1, chip], device))
            sends[-1].start()
        swap.wait()
        for i in range(chips):
            both = mine_image[:, i * LANES : (i + 1) * LANES] + pair_in[step, i].astype(jnp.float32)
            image_f32[i] = both
            chip_out[step, i] = both.astype(jnp.bfloat16)
        for d in range(1, chips):
            other, device = peer(d)
            sends.append(remote(
                chip_out.at[step, other], chip_in.at[step, chip],
                chip_send.at[step, 0, d], chip_recv.at[step, 0, chip], device))
            sends[-1].start()
        for d in range(1, chips):
            other, device = peer(d)
            remote(
                chip_tiles.at[step, other], chip_tiles.at[step, other],
                chip_send.at[step, 1, d], chip_recv.at[step, 1, other], device).wait_recv()
        curve_tile = chip_tiles[step, 0]
        for i in range(1, chips):
            curve_tile = curve_tile + chip_tiles[step, i]
        curvature = unpack_columns(curve_tile, 1, dirs)[0] + damping_term * square
        alpha = norm / curvature
        reduced = image_f32[chip] + damping_term * direction_slice
        for d in range(1, chips):
            other, device = peer(d)
            remote(
                chip_out.at[step, other], chip_in.at[step, other],
                chip_send.at[step, 0, d], chip_recv.at[step, 0, other], device).wait_recv()
            reduced = reduced + chip_in[step, other].astype(jnp.float32)
        resid_slice = resid_slice - alpha * reduced
        gathered[step, core, chip] = resid_slice.astype(jnp.bfloat16)
        spread = []
        for d in range(1, chips):
            other, device = peer(d)
            spread.append(remote(
                gathered.at[step, core, chip], gathered.at[step, core, chip],
                chip_send.at[step, 2, d], chip_recv.at[step, 2, chip], device))
            spread[-1].start()

        def forward(which):
            spread.append(remote(
                gathered.at[step, core, which], gathered.at[step, core, which],
                pair_send.at[step, 2 + which], pair_recv.at[step, 2 + which], partner))
            spread[-1].start()

        forward(chip)
        if step == 0:
            first_alpha = alpha
        else:
            scores = [
                (first_alpha * first_rows[h] + alpha * rows[h]) / math.sqrt(full_width) for h in range(2)
            ]
            scores_ref[...] = jnp.where(feat == 0, scores[0], scores[1])
            for block, lanes in pieces:
                start = targets_ref[:, lanes]
                solution_ref[:, lanes] = first_alpha * start + alpha * (block.astype(jnp.float32) + ratio * start)
        for copy in sends:
            copy.wait_send()
        for d in range(1, chips):
            other, device = peer(d)
            remote(
                gathered.at[step, core, other], gathered.at[step, core, other],
                chip_send.at[step, 2, d], chip_recv.at[step, 2, other], device).wait_recv()
            forward(other)
        if step == ITERS - 1:
            resid_ref[:, own_half] = joined(step, core).astype(jnp.float32)
            for i in range(chips):
                remote(
                    gathered.at[step, 1 - core, i], gathered.at[step, 1 - core, i],
                    pair_send.at[step, 2 + i], pair_recv.at[step, 2 + i], partner).wait_recv()
            resid_ref[:, other_half] = joined(step, 1 - core).astype(jnp.float32)
        for copy in spread:
            copy.wait_send()


def fused(grads, weights, targets):
    rows_dev, feat_cols = grads.shape
    n_samp = lax.axis_size("samp")
    n_feat = lax.axis_size("feat")
    dirs = targets.shape[1]
    chips = n_samp // 2
    f32, b16 = jnp.float32, jnp.bfloat16
    vmem = pl.BlockSpec(memory_space=pltpu.VMEM)
    dma = pltpu.SemaphoreType.DMA
    scores, solved, resid = pl.pallas_call(
        functools.partial(kernel, chips, rows_dev * n_samp, feat_cols * n_feat),
        out_shape=(
            jax.ShapeDtypeStruct((dirs, rows_dev // n_feat), f32),
            jax.ShapeDtypeStruct((dirs, feat_cols), f32),
            jax.ShapeDtypeStruct((dirs, feat_cols), f32),
        ),
        in_specs=[vmem] * 3,
        out_specs=[vmem] * 3,
        scratch_shapes=[
            pltpu.VMEM((ITERS, 2, dirs, rows_dev // 2), b16),
            pltpu.VMEM((ITERS, 2, dirs, rows_dev // 2), b16),
            pltpu.VMEM((ITERS, 8, LANES), f32),
            pltpu.VMEM((ITERS, 8, LANES), f32),
            pltpu.VMEM((chips, dirs, LANES), f32),
            pltpu.VMEM((ITERS, chips, dirs, LANES), b16),
            pltpu.VMEM((ITERS, chips, dirs, LANES), b16),
            pltpu.VMEM((ITERS, 8, LANES), f32),
            pltpu.VMEM((ITERS, 8, LANES), f32),
            pltpu.VMEM((ITERS, chips, dirs, LANES), b16),
            pltpu.VMEM((ITERS, chips, dirs, LANES), b16),
            pltpu.VMEM((ITERS, chips, 8, LANES), f32),
            pltpu.VMEM((ITERS, 2, chips, dirs, LANES), b16),
            dma((ITERS, 3)), dma((ITERS, 3)),
            dma((ITERS, 2 + chips)), dma((ITERS, 2 + chips)),
            dma((ITERS, 3, chips)), dma((ITERS, 3, chips)),
        ],
        compiler_params=pltpu.CompilerParams(collective_id=0, has_side_effects=True, vmem_limit_bytes=VMEM_BYTES),
        name="cg",
    )(grads, weights[None, :], targets.T)
    return scores.T, solved.T, resid.T


def per_device(grads, weights, targets):
    rows_dev, feat_cols = grads.shape
    n_samp = lax.axis_size("samp")
    n_feat = lax.axis_size("feat")
    total = rows_dev * n_samp
    full_width = feat_cols * n_feat
    share = rows_dev // n_feat
    offset = lax.axis_index("feat") * share
    scaled = weights / total
    regrouped = lax.all_to_all(grads, "feat", split_axis=0, concat_axis=1, tiled=True)
    own_weights = lax.dynamic_slice_in_dim(scaled, offset, share, 0)

    def column_norms(resid):
        squares = jnp.sum(resid * resid, axis=0)
        parts = (squares,)
        return lax.psum((parts[0],), "feat")

    solution = jnp.zeros_like(targets)
    resid = targets
    direction = targets
    accum = jnp.zeros((share, targets.shape[1]), jnp.float32)
    norm_now = column_norms(resid)[0]
    for step in range(ITERS):
        packed = direction.astype(jnp.bfloat16)
        sample_rows = jnp.dot(
            regrouped,
            lax.all_gather(packed, "feat", axis=0, tiled=True),
            preferred_element_type=jnp.float32,
        )
        weighted = (sample_rows * own_weights[:, None]).astype(jnp.bfloat16)
        partial_image = lax.psum_scatter(
            lax.dot_general(
                regrouped, weighted, (((0,), (0,)), ((), ())), preferred_element_type=jnp.float32
            ).astype(jnp.bfloat16),
            "feat",
            scatter_dimension=0,
            tiled=True,
        ).astype(jnp.float32)
        own_rows = sample_rows
        apply_own_weights = own_weights
        image = lax.psum(partial_image, "samp") + damping_term * direction
        own_rows, own_weights, image = (own_rows, apply_own_weights, image)
        curvature = lax.psum(jnp.sum(direction * image, axis=0), "feat")
        alpha = norm_now / curvature
        solution = solution + alpha * direction
        resid = resid - alpha * image
        accum = accum + alpha * own_rows
        if step + 1 < ITERS:
            sums = column_norms(resid)
            norm_next = sums[0]
            ratio = norm_next / norm_now
            direction = resid + ratio * direction
            norm_now = norm_next
    scores = accum / math.sqrt(full_width)
    return (scores, solution, resid)


def dispatch(grads, weights, targets):
    rows_dev, feat_cols = grads.shape
    n_samp, n_feat = lax.axis_size("samp"), lax.axis_size("feat")
    fits = (
        n_feat == 2
        and n_samp % 2 == 0
        and n_samp >= 4
        and feat_cols == n_samp * LANES
        and rows_dev % (2 * LANES) == 0
        and targets.shape[1] % 16 == 0
        and targets.shape[1] <= LANES
    )
    return (fused if fits else per_device)(grads, weights, targets)


def solution(mesh):
    return jax.shard_map(
        dispatch,
        mesh=mesh,
        in_specs=(P("samp", "feat"), P("samp"), P("feat", None)),
        out_specs=(P(("samp", "feat"), None), P("feat", None), P("feat", None)),
        check_vma=False,
    )
```

```python
import functools
import math

import jax
import jax.numpy as jnp
from jax import lax
from jax.experimental import pallas as pl
from jax.experimental.pallas import tpu as pltpu
from jax.sharding import PartitionSpec as P

ITERS = 2
LANES = 128
BATCHES = 2
VMEM_BYTES = 16 * 2**20
MESH = pl.DeviceIdType.MESH

damping_term = 0.1


def pack_columns(columns):
    dirs = columns[0].shape[0]
    lane = lax.broadcasted_iota(jnp.int32, (dirs, LANES), 1)
    tile = jnp.zeros((dirs, LANES), jnp.float32)
    for position, column in enumerate(columns):
        tile = jnp.where(lane == position, column, tile)
    if dirs < LANES:
        tile = jnp.concatenate([tile, jnp.zeros((LANES - dirs, LANES), jnp.float32)], axis=0)
    return tile.T[:8]


def unpack_columns(tile, count, dirs):
    padded = jnp.concatenate([tile, jnp.zeros((LANES - 8, LANES), jnp.float32)], axis=0).T
    return [padded[:dirs, i : i + 1] for i in range(count)]


def kernel(
    chips, total, full_width,
    grads_ref, weights_ref, targets_ref,
    scores_ref, solution_ref, resid_ref,
    rows_out, rows_in, tile_out, tile_in,
    image_f32, image_b16, pair_in, pair_tile_out, pair_tile_in,
    chip_out, chip_in, chip_tiles, gathered,
    feat_send, feat_recv, pair_send, pair_recv, chip_send, chip_recv,
):
    samp, feat = lax.axis_index("samp"), lax.axis_index("feat")
    core = lax.rem(samp, 2)
    chip = lax.div(samp, 2)
    dirs = targets_ref.shape[0] // BATCHES
    rows_dev = grads_ref.shape[0]
    half = rows_dev // 2
    partner = (samp + 1 - 2 * core, feat)
    mirror = (samp, 1 - feat)
    wide_half = chips * LANES

    def peer(offset):
        other = lax.rem(chip + offset, chips)
        return other, (other * 2 + core, feat)

    barrier = pltpu.get_barrier_semaphore()
    for device in [partner, mirror] + [peer(d)[1] for d in range(1, chips)]:
        pl.semaphore_signal(barrier, inc=1, device_id=device, device_id_type=MESH)

    def remote(src, dst, send, recv, device):
        return pltpu.make_async_remote_copy(
            src_ref=src, dst_ref=dst, send_sem=send, recv_sem=recv, device_id=device, device_id_type=MESH
        )

    def lanes_of(which):
        return pl.ds(pl.multiple_of(which * wide_half, wide_half), wide_half)

    own_half, other_half = lanes_of(core), lanes_of(1 - core)
    own_lanes = pl.ds(pl.multiple_of((core * chips + chip) * LANES, LANES), LANES)
    nt = (((1,), (1,)), ((), ()))

    def joined(step, which):
        return jnp.concatenate([gathered[step, which, i] for i in range(chips)], axis=1)

    def solve(batch):
        lines = slice(batch * dirs, (batch + 1) * dirs)
        for step in range(ITERS):
            at = step * BATCHES + batch
            mine = []
            copies = []
            if step == 0:
                targets = targets_ref[lines, :]
                packed = targets.astype(jnp.bfloat16)
            else:
                near = joined(at - BATCHES, core)
                started = [
                    lax.dot_general(
                        near, grads_ref[h * half : (h + 1) * half, own_half], nt,
                        preferred_element_type=jnp.float32)
                    for h in range(2)
                ]
                yield
                for i in range(chips):
                    remote(
                        gathered.at[at - BATCHES, 1 - core, i], gathered.at[at - BATCHES, 1 - core, i],
                        pair_send.at[at - BATCHES, 2 + i], pair_recv.at[at - BATCHES, 2 + i], partner).wait_recv()
                far = joined(at - BATCHES, 1 - core)
            for h in range(2):
                rows_h = slice(h * half, (h + 1) * half)
                if step == 0:
                    part = lax.dot_general(
                        packed, grads_ref[rows_h, :], nt, preferred_element_type=jnp.float32)
                else:
                    part = started[h] + lax.dot_general(
                        far, grads_ref[rows_h, other_half], nt, preferred_element_type=jnp.float32)
                rows_out[at, h] = part.astype(jnp.bfloat16)
                if step == 0 and h == 0 and batch == 0:
                    pl.semaphore_wait(barrier, chips + 1)
                copies.append(remote(
                    rows_out.at[at, h], rows_in.at[at, h],
                    feat_send.at[at, h], feat_recv.at[at, h], mirror))
                copies[-1].start()
                mine.append(part)
            if step == 0:
                sums = [jnp.sum(targets * targets, axis=1, keepdims=True)]
            else:
                pieces = [(near, own_half), (far, other_half)]
                sums = [0.0, 0.0]
                for block, lanes in pieces:
                    block = block.astype(jnp.float32)
                    sums[0] = sums[0] + jnp.sum(block * block, axis=1, keepdims=True)
                    sums[1] = sums[1] + jnp.sum(block * targets_ref[lines, lanes], axis=1, keepdims=True)
            tile_out[at] = pack_columns(sums)
            copies.append(remote(tile_out.at[at], tile_in.at[at], feat_send.at[at, 2], feat_recv.at[at, 2], mirror))
            copies[-1].start()
            if step == 0:
                scaled = weights_ref[...] / total
                target_slice = targets_ref[lines, own_lanes]

            def finish_sums():
                copies[2].wait()
                return unpack_columns(tile_out[at] + tile_in[at], len(sums), dirs)

            yield
            if step == 1:
                sums = finish_sums()
                norm = sums[0]
                ratio = norm / first_norm
                square = norm + 2.0 * ratio * sums[1] + ratio * ratio * first_norm
                direction_slice = resid_slice + ratio * target_slice
            rows, curve = [], 0.0
            toward = mine_image = None
            for h in range(2):
                rows_h = slice(h * half, (h + 1) * half)
                copies[h].wait()
                whole = mine[h] + rows_in[at, h].astype(jnp.float32)
                if step == 1:
                    whole = whole + ratio * first_rows[h]
                rows.append(whole)
                weighted = (whole * scaled[:, rows_h]).astype(jnp.bfloat16)
                there = jnp.dot(weighted, grads_ref[rows_h, other_half], preferred_element_type=jnp.float32)
                toward = there if h == 0 else toward + there
                if h == 1:
                    for i in range(chips):
                        image_b16[at, i] = toward[:, i * LANES : (i + 1) * LANES].astype(jnp.bfloat16)
                    swap = remote(image_b16.at[at], pair_in.at[at], pair_send.at[at, 0], pair_recv.at[at, 0], partner)
                    swap.start()
                curve = curve + jnp.sum(weighted.astype(jnp.float32) * whole, axis=1, keepdims=True)
                if h == 1:
                    pair_tile_out[at] = pack_columns([curve])
                    swap_tile = remote(
                        pair_tile_out.at[at], pair_tile_in.at[at], pair_send.at[at, 1], pair_recv.at[at, 1], partner)
                    swap_tile.start()
                here = jnp.dot(weighted, grads_ref[rows_h, own_half], preferred_element_type=jnp.float32)
                mine_image = here if h == 0 else mine_image + here
            if step == 0:
                first_rows = rows
                sums = finish_sums()
                first_norm = norm = square = sums[0]
                resid_slice = direction_slice = target_slice
            yield
            swap_tile.wait()
            chip_tiles[at, chip] = pair_tile_out[at] + pair_tile_in[at]
            sends = []
            for d in range(1, chips):
                other, device = peer(d)
                sends.append(remote(
                    chip_tiles.at[at, chip], chip_tiles.at[at, chip],
                    chip_send.at[at, 1, d], chip_recv.at[at, 1, chip], device))
                sends[-1].start()
            swap.wait()
            for i in range(chips):
                both = mine_image[:, i * LANES : (i + 1) * LANES] + pair_in[at, i].astype(jnp.float32)
                image_f32[batch, i] = both
                chip_out[at, i] = both.astype(jnp.bfloat16)
            for d in range(1, chips):
                other, device = peer(d)
                sends.append(remote(
                    chip_out.at[at, other], chip_in.at[at, chip],
                    chip_send.at[at, 0, d], chip_recv.at[at, 0, chip], device))
                sends[-1].start()
            yield
            for d in range(1, chips):
                other, device = peer(d)
                remote(
                    chip_tiles.at[at, other], chip_tiles.at[at, other],
                    chip_send.at[at, 1, d], chip_recv.at[at, 1, other], device).wait_recv()
            curve_tile = chip_tiles[at, 0]
            for i in range(1, chips):
                curve_tile = curve_tile + chip_tiles[at, i]
            curvature = unpack_columns(curve_tile, 1, dirs)[0] + damping_term * square
            alpha = norm / curvature
            reduced = image_f32[batch, chip] + damping_term * direction_slice
            for d in range(1, chips):
                other, device = peer(d)
                remote(
                    chip_out.at[at, other], chip_in.at[at, other],
                    chip_send.at[at, 0, d], chip_recv.at[at, 0, other], device).wait_recv()
                reduced = reduced + chip_in[at, other].astype(jnp.float32)
            resid_slice = resid_slice - alpha * reduced
            gathered[at, core, chip] = resid_slice.astype(jnp.bfloat16)
            spread = []
            for d in range(1, chips):
                other, device = peer(d)
                spread.append(remote(
                    gathered.at[at, core, chip], gathered.at[at, core, chip],
                    chip_send.at[at, 2, d], chip_recv.at[at, 2, chip], device))
                spread[-1].start()

            def forward(which):
                spread.append(remote(
                    gathered.at[at, core, which], gathered.at[at, core, which],
                    pair_send.at[at, 2 + which], pair_recv.at[at, 2 + which], partner))
                spread[-1].start()

            forward(chip)
            if step == 0:
                first_alpha = alpha
            else:
                scores = [
                    (first_alpha * first_rows[h] + alpha * rows[h]) / math.sqrt(full_width) for h in range(2)
                ]
                scores_ref[lines, :] = jnp.where(feat == 0, scores[0], scores[1])
                for block, lanes in pieces:
                    start = targets_ref[lines, lanes]
                    solution_ref[lines, lanes] = first_alpha * start + alpha * (block.astype(jnp.float32) + ratio * start)
            yield
            for copy in sends:
                copy.wait_send()
            for d in range(1, chips):
                other, device = peer(d)
                remote(
                    gathered.at[at, core, other], gathered.at[at, core, other],
                    chip_send.at[at, 2, d], chip_recv.at[at, 2, other], device).wait_recv()
                forward(other)
            if step == ITERS - 1:
                resid_ref[lines, own_half] = joined(at, core).astype(jnp.float32)
                yield
                for i in range(chips):
                    remote(
                        gathered.at[at, 1 - core, i], gathered.at[at, 1 - core, i],
                        pair_send.at[at, 2 + i], pair_recv.at[at, 2 + i], partner).wait_recv()
                resid_ref[lines, other_half] = joined(at, 1 - core).astype(jnp.float32)
            for copy in spread:
                copy.wait_send()

    running = [solve(batch) for batch in range(BATCHES)]
    while running:
        running = [one for one in running if next(one, True) is None]


def fused(grads, weights, targets):
    rows_dev, feat_cols = grads.shape
    n_samp = lax.axis_size("samp")
    n_feat = lax.axis_size("feat")
    dirs = targets.shape[1]
    slots, lines = ITERS * BATCHES, dirs // BATCHES
    chips = n_samp // 2
    f32, b16 = jnp.float32, jnp.bfloat16
    vmem = pl.BlockSpec(memory_space=pltpu.VMEM)
    dma = pltpu.SemaphoreType.DMA
    scores, solved, resid = pl.pallas_call(
        functools.partial(kernel, chips, rows_dev * n_samp, feat_cols * n_feat),
        out_shape=(
            jax.ShapeDtypeStruct((dirs, rows_dev // n_feat), f32),
            jax.ShapeDtypeStruct((dirs, feat_cols), f32),
            jax.ShapeDtypeStruct((dirs, feat_cols), f32),
        ),
        in_specs=[vmem] * 3,
        out_specs=[vmem] * 3,
        scratch_shapes=[
            pltpu.VMEM((slots, 2, lines, rows_dev // 2), b16),
            pltpu.VMEM((slots, 2, lines, rows_dev // 2), b16),
            pltpu.VMEM((slots, 8, LANES), f32),
            pltpu.VMEM((slots, 8, LANES), f32),
            pltpu.VMEM((BATCHES, chips, lines, LANES), f32),
            pltpu.VMEM((slots, chips, lines, LANES), b16),
            pltpu.VMEM((slots, chips, lines, LANES), b16),
            pltpu.VMEM((slots, 8, LANES), f32),
            pltpu.VMEM((slots, 8, LANES), f32),
            pltpu.VMEM((slots, chips, lines, LANES), b16),
            pltpu.VMEM((slots, chips, lines, LANES), b16),
            pltpu.VMEM((slots, chips, 8, LANES), f32),
            pltpu.VMEM((slots, 2, chips, lines, LANES), b16),
            dma((slots, 3)), dma((slots, 3)),
            dma((slots, 2 + chips)), dma((slots, 2 + chips)),
            dma((slots, 3, chips)), dma((slots, 3, chips)),
        ],
        compiler_params=pltpu.CompilerParams(collective_id=0, has_side_effects=True, vmem_limit_bytes=VMEM_BYTES),
        name="cg",
    )(grads, weights[None, :], targets.T)
    return scores.T, solved.T, resid.T


def per_device(grads, weights, targets):
    rows_dev, feat_cols = grads.shape
    n_samp = lax.axis_size("samp")
    n_feat = lax.axis_size("feat")
    total = rows_dev * n_samp
    full_width = feat_cols * n_feat
    share = rows_dev // n_feat
    offset = lax.axis_index("feat") * share
    scaled = weights / total
    regrouped = lax.all_to_all(grads, "feat", split_axis=0, concat_axis=1, tiled=True)
    own_weights = lax.dynamic_slice_in_dim(scaled, offset, share, 0)

    def column_norms(resid):
        squares = jnp.sum(resid * resid, axis=0)
        parts = (squares,)
        return lax.psum((parts[0],), "feat")

    solution = jnp.zeros_like(targets)
    resid = targets
    direction = targets
    accum = jnp.zeros((share, targets.shape[1]), jnp.float32)
    norm_now = column_norms(resid)[0]
    for step in range(ITERS):
        packed = direction.astype(jnp.bfloat16)
        sample_rows = jnp.dot(
            regrouped,
            lax.all_gather(packed, "feat", axis=0, tiled=True),
            preferred_element_type=jnp.float32,
        )
        weighted = (sample_rows * own_weights[:, None]).astype(jnp.bfloat16)
        partial_image = lax.psum_scatter(
            lax.dot_general(
                regrouped, weighted, (((0,), (0,)), ((), ())), preferred_element_type=jnp.float32
            ).astype(jnp.bfloat16),
            "feat",
            scatter_dimension=0,
            tiled=True,
        ).astype(jnp.float32)
        own_rows = sample_rows
        apply_own_weights = own_weights
        image = lax.psum(partial_image, "samp") + damping_term * direction
        own_rows, own_weights, image = (own_rows, apply_own_weights, image)
        curvature = lax.psum(jnp.sum(direction * image, axis=0), "feat")
        alpha = norm_now / curvature
        solution = solution + alpha * direction
        resid = resid - alpha * image
        accum = accum + alpha * own_rows
        if step + 1 < ITERS:
            sums = column_norms(resid)
            norm_next = sums[0]
            ratio = norm_next / norm_now
            direction = resid + ratio * direction
            norm_now = norm_next
    scores = accum / math.sqrt(full_width)
    return (scores, solution, resid)


def dispatch(grads, weights, targets):
    rows_dev, feat_cols = grads.shape
    n_samp, n_feat = lax.axis_size("samp"), lax.axis_size("feat")
    fits = (
        n_feat == 2
        and n_samp % 2 == 0
        and n_samp >= 4
        and feat_cols == n_samp * LANES
        and rows_dev % (2 * LANES) == 0
        and targets.shape[1] % (16 * BATCHES) == 0
        and targets.shape[1] <= LANES
    )
    return (fused if fits else per_device)(grads, weights, targets)


def solution(mesh):
    return jax.shard_map(
        dispatch,
        mesh=mesh,
        in_specs=(P("samp", "feat"), P("samp"), P("feat", None)),
        out_specs=(P(("samp", "feat"), None), P("feat", None), P("feat", None)),
        check_vma=False,
    )
```

```python
import functools
import math

import jax
import jax.numpy as jnp
from jax import lax
from jax.experimental import pallas as pl
from jax.experimental.pallas import tpu as pltpu
from jax.sharding import PartitionSpec as P

ITERS = 2
LANES = 128
VMEM_BYTES = 105 * 2**19
MESH = pl.DeviceIdType.MESH

damping_term = 0.1


def pack_columns(columns):
    dirs = columns[0].shape[0]
    lane = lax.broadcasted_iota(jnp.int32, (dirs, LANES), 1)
    tile = jnp.zeros((dirs, LANES), jnp.float32)
    for position, column in enumerate(columns):
        tile = jnp.where(lane == position, column, tile)
    if dirs < LANES:
        tile = jnp.concatenate([tile, jnp.zeros((LANES - dirs, LANES), jnp.float32)], axis=0)
    return tile.T[:8]


def unpack_columns(tile, count, dirs):
    padded = jnp.concatenate([tile, jnp.zeros((LANES - 8, LANES), jnp.float32)], axis=0).T
    return [padded[:dirs, i : i + 1] for i in range(count)]


def kernel(
    chips, total, full_width,
    grads_hbm, weights_hbm, targets_hbm,
    scores_ref, solution_ref, resid_ref,
    grads_ref, weights_ref, targets_ref,
    rows_out, rows_in, tile_out, tile_in,
    image_f32, image_b16, pair_in, pair_tile_out, pair_tile_in,
    chip_out, chip_in, chip_tiles, gathered,
    load_sem, feat_send, feat_recv, pair_send, pair_recv, chip_send, chip_recv,
):
    samp, feat = lax.axis_index("samp"), lax.axis_index("feat")
    core = lax.rem(samp, 2)
    chip = lax.div(samp, 2)
    dirs, width = targets_ref.shape
    rows_dev = grads_ref.shape[0]
    half = rows_dev // 2
    partner = (samp + 1 - 2 * core, feat)
    mirror = (samp, 1 - feat)
    wide_half = chips * LANES

    def peer(offset):
        other = lax.rem(chip + offset, chips)
        return other, (other * 2 + core, feat)

    loads = [
        pltpu.make_async_copy(targets_hbm, targets_ref, load_sem.at[0]),
        pltpu.make_async_copy(grads_hbm.at[pl.ds(0, half)], grads_ref.at[pl.ds(0, half)], load_sem.at[1]),
        pltpu.make_async_copy(grads_hbm.at[pl.ds(half, half)], grads_ref.at[pl.ds(half, half)], load_sem.at[2]),
        pltpu.make_async_copy(weights_hbm, weights_ref, load_sem.at[3]),
    ]
    for load in loads:
        load.start()

    barrier = pltpu.get_barrier_semaphore()
    for device in [partner, mirror] + [peer(d)[1] for d in range(1, chips)]:
        pl.semaphore_signal(barrier, inc=1, device_id=device, device_id_type=MESH)

    def remote(src, dst, send, recv, device):
        return pltpu.make_async_remote_copy(
            src_ref=src, dst_ref=dst, send_sem=send, recv_sem=recv, device_id=device, device_id_type=MESH
        )

    def lanes_of(which):
        return pl.ds(pl.multiple_of(which * wide_half, wide_half), wide_half)

    own_half, other_half = lanes_of(core), lanes_of(1 - core)
    own_lanes = pl.ds(pl.multiple_of((core * chips + chip) * LANES, LANES), LANES)
    nt = (((1,), (1,)), ((), ()))

    def joined(step, which):
        return jnp.concatenate([gathered[step, which, i] for i in range(chips)], axis=1)

    for step in range(ITERS):
        mine = []
        copies = []
        if step == 0:
            loads[0].wait()
            targets = targets_ref[...]
            packed = targets.astype(jnp.bfloat16)
        else:
            near = joined(step - 1, core)
            started = [
                lax.dot_general(
                    near, grads_ref[h * half : (h + 1) * half, own_half], nt,
                    preferred_element_type=jnp.float32)
                for h in range(2)
            ]
            for i in range(chips):
                remote(
                    gathered.at[step - 1, 1 - core, i], gathered.at[step - 1, 1 - core, i],
                    pair_send.at[step - 1, 2 + i], pair_recv.at[step - 1, 2 + i], partner).wait_recv()
            far = joined(step - 1, 1 - core)
        for h in range(2):
            rows_h = slice(h * half, (h + 1) * half)
            if step == 0:
                loads[1 + h].wait()
                part = lax.dot_general(
                    packed, grads_ref[rows_h, :], nt, preferred_element_type=jnp.float32)
            else:
                part = started[h] + lax.dot_general(
                    far, grads_ref[rows_h, other_half], nt, preferred_element_type=jnp.float32)
            rows_out[step, h] = part.astype(jnp.bfloat16)
            if step == 0 and h == 0:
                pl.semaphore_wait(barrier, chips + 1)
            copies.append(remote(
                rows_out.at[step, h], rows_in.at[step, h],
                feat_send.at[step, h], feat_recv.at[step, h], mirror))
            copies[-1].start()
            mine.append(part)
        if step == 0:
            sums = [jnp.sum(targets * targets, axis=1, keepdims=True)]
        else:
            pieces = [(near, own_half), (far, other_half)]
            sums = [0.0, 0.0]
            for block, lanes in pieces:
                block = block.astype(jnp.float32)
                sums[0] = sums[0] + jnp.sum(block * block, axis=1, keepdims=True)
                sums[1] = sums[1] + jnp.sum(block * targets_ref[:, lanes], axis=1, keepdims=True)
        tile_out[step] = pack_columns(sums)
        copies.append(remote(tile_out.at[step], tile_in.at[step], feat_send.at[step, 2], feat_recv.at[step, 2], mirror))
        copies[-1].start()
        if step == 0:
            loads[3].wait()
            scaled = weights_ref[...] / total
            target_slice = targets_ref[:, own_lanes]

        def finish_sums():
            copies[2].wait()
            return unpack_columns(tile_out[step] + tile_in[step], len(sums), dirs)

        if step == 1:
            sums = finish_sums()
            norm = sums[0]
            ratio = norm / first_norm
            square = norm + 2.0 * ratio * sums[1] + ratio * ratio * first_norm
            direction_slice = resid_slice + ratio * target_slice
        rows, curve = [], 0.0
        toward = mine_image = None
        for h in range(2):
            rows_h = slice(h * half, (h + 1) * half)
            copies[h].wait()
            whole = mine[h] + rows_in[step, h].astype(jnp.float32)
            if step == 1:
                whole = whole + ratio * first_rows[h]
            rows.append(whole)
            weighted = (whole * scaled[:, rows_h]).astype(jnp.bfloat16)
            there = jnp.dot(weighted, grads_ref[rows_h, other_half], preferred_element_type=jnp.float32)
            toward = there if h == 0 else toward + there
            if h == 1:
                for i in range(chips):
                    image_b16[step, i] = toward[:, i * LANES : (i + 1) * LANES].astype(jnp.bfloat16)
                swap = remote(image_b16.at[step], pair_in.at[step], pair_send.at[step, 0], pair_recv.at[step, 0], partner)
                swap.start()
            curve = curve + jnp.sum(weighted.astype(jnp.float32) * whole, axis=1, keepdims=True)
            if h == 1:
                pair_tile_out[step] = pack_columns([curve])
                swap_tile = remote(
                    pair_tile_out.at[step], pair_tile_in.at[step], pair_send.at[step, 1], pair_recv.at[step, 1], partner)
                swap_tile.start()
            here = jnp.dot(weighted, grads_ref[rows_h, own_half], preferred_element_type=jnp.float32)
            mine_image = here if h == 0 else mine_image + here
        if step == 0:
            first_rows = rows
            sums = finish_sums()
            first_norm = norm = square = sums[0]
            resid_slice = direction_slice = target_slice
        swap_tile.wait()
        chip_tiles[step, chip] = pair_tile_out[step] + pair_tile_in[step]
        sends = []
        for d in range(1, chips):
            other, device = peer(d)
            sends.append(remote(
                chip_tiles.at[step, chip], chip_tiles.at[step, chip],
                chip_send.at[step, 1, d], chip_recv.at[step, 1, chip], device))
            sends[-1].start()
        swap.wait()
        for i in range(chips):
            both = mine_image[:, i * LANES : (i + 1) * LANES] + pair_in[step, i].astype(jnp.float32)
            image_f32[i] = both
            chip_out[step, i] = both.astype(jnp.bfloat16)
        for d in range(1, chips):
            other, device = peer(d)
            sends.append(remote(
                chip_out.at[step, other], chip_in.at[step, chip],
                chip_send.at[step, 0, d], chip_recv.at[step, 0, chip], device))
            sends[-1].start()
        for d in range(1, chips):
            other, device = peer(d)
            remote(
                chip_tiles.at[step, other], chip_tiles.at[step, other],
                chip_send.at[step, 1, d], chip_recv.at[step, 1, other], device).wait_recv()
        curve_tile = chip_tiles[step, 0]
        for i in range(1, chips):
            curve_tile = curve_tile + chip_tiles[step, i]
        curvature = unpack_columns(curve_tile, 1, dirs)[0] + damping_term * square
        alpha = norm / curvature
        reduced = image_f32[chip] + damping_term * direction_slice
        for d in range(1, chips):
            other, device = peer(d)
            remote(
                chip_out.at[step, other], chip_in.at[step, other],
                chip_send.at[step, 0, d], chip_recv.at[step, 0, other], device).wait_recv()
            reduced = reduced + chip_in[step, other].astype(jnp.float32)
        resid_slice = resid_slice - alpha * reduced
        gathered[step, core, chip] = resid_slice.astype(jnp.bfloat16)
        spread = []
        for d in range(1, chips):
            other, device = peer(d)
            spread.append(remote(
                gathered.at[step, core, chip], gathered.at[step, core, chip],
                chip_send.at[step, 2, d], chip_recv.at[step, 2, chip], device))
            spread[-1].start()

        def forward(which):
            spread.append(remote(
                gathered.at[step, core, which], gathered.at[step, core, which],
                pair_send.at[step, 2 + which], pair_recv.at[step, 2 + which], partner))
            spread[-1].start()

        forward(chip)
        if step == 0:
            first_alpha = alpha
        else:
            scores = [
                (first_alpha * first_rows[h] + alpha * rows[h]) / math.sqrt(full_width) for h in range(2)
            ]
            scores_ref[...] = jnp.where(feat == 0, scores[0], scores[1])
            for block, lanes in pieces:
                start = targets_ref[:, lanes]
                solution_ref[:, lanes] = first_alpha * start + alpha * (block.astype(jnp.float32) + ratio * start)
        for copy in sends:
            copy.wait_send()
        for d in range(1, chips):
            other, device = peer(d)
            remote(
                gathered.at[step, core, other], gathered.at[step, core, other],
                chip_send.at[step, 2, d], chip_recv.at[step, 2, other], device).wait_recv()
            forward(other)
        if step == ITERS - 1:
            resid_ref[:, own_half] = joined(step, core).astype(jnp.float32)
            for i in range(chips):
                remote(
                    gathered.at[step, 1 - core, i], gathered.at[step, 1 - core, i],
                    pair_send.at[step, 2 + i], pair_recv.at[step, 2 + i], partner).wait_recv()
            resid_ref[:, other_half] = joined(step, 1 - core).astype(jnp.float32)
        for copy in spread:
            copy.wait_send()


def fused(grads, weights, targets):
    rows_dev, feat_cols = grads.shape
    n_samp = lax.axis_size("samp")
    n_feat = lax.axis_size("feat")
    dirs = targets.shape[1]
    chips = n_samp // 2
    f32, b16 = jnp.float32, jnp.bfloat16
    vmem = pl.BlockSpec(memory_space=pltpu.VMEM)
    dma = pltpu.SemaphoreType.DMA
    scores, solved, resid = pl.pallas_call(
        functools.partial(kernel, chips, rows_dev * n_samp, feat_cols * n_feat),
        out_shape=(
            jax.ShapeDtypeStruct((dirs, rows_dev // n_feat), f32),
            jax.ShapeDtypeStruct((dirs, feat_cols), f32),
            jax.ShapeDtypeStruct((dirs, feat_cols), f32),
        ),
        in_specs=[pl.BlockSpec(memory_space=pltpu.HBM)] * 3,
        out_specs=[vmem] * 3,
        scratch_shapes=[
            pltpu.VMEM((rows_dev, feat_cols), b16),
            pltpu.VMEM((1, rows_dev), f32),
            pltpu.VMEM((dirs, feat_cols), f32),
            pltpu.VMEM((ITERS, 2, dirs, rows_dev // 2), b16),
            pltpu.VMEM((ITERS, 2, dirs, rows_dev // 2), b16),
            pltpu.VMEM((ITERS, 8, LANES), f32),
            pltpu.VMEM((ITERS, 8, LANES), f32),
            pltpu.VMEM((chips, dirs, LANES), f32),
            pltpu.VMEM((ITERS, chips, dirs, LANES), b16),
            pltpu.VMEM((ITERS, chips, dirs, LANES), b16),
            pltpu.VMEM((ITERS, 8, LANES), f32),
            pltpu.VMEM((ITERS, 8, LANES), f32),
            pltpu.VMEM((ITERS, chips, dirs, LANES), b16),
            pltpu.VMEM((ITERS, chips, dirs, LANES), b16),
            pltpu.VMEM((ITERS, chips, 8, LANES), f32),
            pltpu.VMEM((ITERS, 2, chips, dirs, LANES), b16),
            dma((4,)),
            dma((ITERS, 3)), dma((ITERS, 3)),
            dma((ITERS, 2 + chips)), dma((ITERS, 2 + chips)),
            dma((ITERS, 3, chips)), dma((ITERS, 3, chips)),
        ],
        compiler_params=pltpu.CompilerParams(collective_id=0, has_side_effects=True, vmem_limit_bytes=VMEM_BYTES),
        name="cg",
    )(grads, weights[None, :], targets.T)
    return scores.T, solved.T, resid.T


def per_device(grads, weights, targets):
    rows_dev, feat_cols = grads.shape
    n_samp = lax.axis_size("samp")
    n_feat = lax.axis_size("feat")
    total = rows_dev * n_samp
    full_width = feat_cols * n_feat
    share = rows_dev // n_feat
    offset = lax.axis_index("feat") * share
    scaled = weights / total
    regrouped = lax.all_to_all(grads, "feat", split_axis=0, concat_axis=1, tiled=True)
    own_weights = lax.dynamic_slice_in_dim(scaled, offset, share, 0)

    def column_norms(resid):
        squares = jnp.sum(resid * resid, axis=0)
        parts = (squares,)
        return lax.psum((parts[0],), "feat")

    solution = jnp.zeros_like(targets)
    resid = targets
    direction = targets
    accum = jnp.zeros((share, targets.shape[1]), jnp.float32)
    norm_now = column_norms(resid)[0]
    for step in range(ITERS):
        packed = direction.astype(jnp.bfloat16)
        sample_rows = jnp.dot(
            regrouped,
            lax.all_gather(packed, "feat", axis=0, tiled=True),
            preferred_element_type=jnp.float32,
        )
        weighted = (sample_rows * own_weights[:, None]).astype(jnp.bfloat16)
        partial_image = lax.psum_scatter(
            lax.dot_general(
                regrouped, weighted, (((0,), (0,)), ((), ())), preferred_element_type=jnp.float32
            ).astype(jnp.bfloat16),
            "feat",
            scatter_dimension=0,
            tiled=True,
        ).astype(jnp.float32)
        own_rows = sample_rows
        apply_own_weights = own_weights
        image = lax.psum(partial_image, "samp") + damping_term * direction
        own_rows, own_weights, image = (own_rows, apply_own_weights, image)
        curvature = lax.psum(jnp.sum(direction * image, axis=0), "feat")
        alpha = norm_now / curvature
        solution = solution + alpha * direction
        resid = resid - alpha * image
        accum = accum + alpha * own_rows
        if step + 1 < ITERS:
            sums = column_norms(resid)
            norm_next = sums[0]
            ratio = norm_next / norm_now
            direction = resid + ratio * direction
            norm_now = norm_next
    scores = accum / math.sqrt(full_width)
    return (scores, solution, resid)


def dispatch(grads, weights, targets):
    rows_dev, feat_cols = grads.shape
    n_samp, n_feat = lax.axis_size("samp"), lax.axis_size("feat")
    fits = (
        n_feat == 2
        and n_samp % 2 == 0
        and n_samp >= 4
        and feat_cols == n_samp * LANES
        and rows_dev % (2 * LANES) == 0
        and targets.shape[1] % 16 == 0
        and targets.shape[1] <= LANES
    )
    return (fused if fits else per_device)(grads, weights, targets)


def solution(mesh):
    return jax.shard_map(
        dispatch,
        mesh=mesh,
        in_specs=(P("samp", "feat"), P("samp"), P("feat", None)),
        out_specs=(P(("samp", "feat"), None), P("feat", None), P("feat", None)),
        check_vma=False,
    )
```
